1024 devices in a mesh: expert: 64 (over z_lo, x), replica: 16 (over z_hi, y, core).
Axes of the slice: x: 4, y: 4, z: 32 (z_hi: 2, z_lo: 16; z = z_hi * 16 + z_lo), core: 2. Of those that a mesh axis runs over, the one named last changes fastest.
Arguments:
- a_tokens: bfloat16 [65536, 2048], P(('expert', 'replica')), may hold values from -6 to 6
- a_ids: int32 [65536, 6], P(('expert', 'replica')), may hold values from 0 to 63, all different within a row
- a_gates: float32 [65536, 6], P(('expert', 'replica')), may hold values from 0.05 to 0.6
- a_valid: int32 [65536], P(('expert', 'replica')), may hold values 0 or 1
- b_cot: bfloat16 [65536, 2048], P(('expert', 'replica')), may hold values from -1.25 to 1.25
- b_ids: int32 [65536, 6], P(('expert', 'replica')), may hold values from 0 to 63, all different within a row
- b_gates: float32 [65536, 6], P(('expert', 'replica')), may hold values from 0.05 to 0.6
- b_valid: int32 [65536], P(('expert', 'replica')), may hold values 0 or 1
- b_hidden: bfloat16 [64, 6144, 704], P('expert', 'replica'), may hold values from -6 to 6
- w_gate: bfloat16 [64, 2048, 704], P('expert'), may hold values from -0.125 to 0.125
- w_up: bfloat16 [64, 2048, 704], P('expert'), may hold values from -0.125 to 0.125
- w_down: bfloat16 [64, 704, 2048], P('expert'), may hold values from -0.21875 to 0.21875
Outputs:
- a_out: bfloat16 [65536, 2048], P(('expert', 'replica'))
- grad_down: float32 [64, 704, 2048], P('expert', None, 'replica')
The draws below stay inside these ranges and needn't reach their ends.
Inputs may be any that keep to these rules, and one draw needn't show every extreme that they name: `a_ids`: each token names 6 different experts. `b_ids`: each token names 6 different experts.
All inputs are finite; a program needn't handle non-finite values. No bound on the sum of `a_valid` or of `b_valid` on one device may be relied on, other than what follows from the above.
Results may differ from the reference program's by a relative error of at most 0.012.
Values may be sent and summed in bfloat16 or wider, within the bound.
A program may use at most 64 MiB of HBM per device.

```python
import math
from functools import partial
import jax
import jax.numpy as jnp
from jax import lax

D = 2048
FW = 704
TOP = 6
TOK_DEV = 64
EXPERTS = 64
CAP = 6
TOKENS = 65536
SLOTS = 6144
N_EXPERT = 64
N_REPLICA = 16


def touch_ends(drawn, rng, smallest, top_value):
    longest = drawn.shape.index(max(drawn.shape))
    spots = []
    for shift in (0, 1):
        where = [jax.random.randint(jax.random.fold_in(rng, axis), (), 0, length) for axis, length in enumerate(drawn.shape)]
        where[longest] = (where[longest] + shift) % drawn.shape[longest]
        spots.append(tuple(where))
    return drawn.at[spots[0]].set(smallest).at[spots[1]].set(top_value)


def spiked(entries, stream_key, source, target, blocks, factor):
    owner, partner = [(jnp.arange(entries.shape[dim]) // (entries.shape[dim] // blocks)).reshape([-1 if axis == dim else 1 for axis in range(entries.ndim)]) for dim in (source, target)]
    chosen = jax.random.permutation(stream_key, blocks)[partner]
    strong = (owner == chosen) | (owner == (partner + blocks // 2) % blocks)
    return jnp.where(strong, factor * entries, entries)


def levels(stream_key, dims, split, least, largest):
    factor_of, own = 1.0, jax.random.fold_in(stream_key, 6)
    for dim, shards_of in split:
        steps = jnp.exp(jax.random.uniform(jax.random.fold_in(own, dim), (shards_of,), jnp.float32, least / len(split), largest / len(split)))
        factor_of = factor_of * jnp.repeat(steps, dims[dim] // shards_of).reshape([-1 if axis == dim else 1 for axis in range(len(dims))])
    return factor_of


def distinct(stream_key, rows, number_of, top, lift):
    sequence = jax.random.permutation(jax.random.fold_in(stream_key, 1), number_of)
    boost = sequence
    for power in range(3):
        boost = boost * boost // number_of
    boost = boost * lift // number_of
    tickets = jax.random.randint(jax.random.fold_in(stream_key, 2), (rows, number_of), 0, 4096) + boost
    fixed_rows = jax.random.permutation(jax.random.fold_in(stream_key, 3), rows)[jnp.arange(number_of) % rows]
    tickets = jnp.where(jnp.arange(rows)[:, None] == fixed_rows[None, :], 1 << 14, tickets)
    score = tickets * number_of + jnp.arange(number_of)
    return lax.top_k(score.astype(jnp.int32), top)[1].astype(jnp.int32)


def noise(own_key, extent, deviation, reach, cuts=(), kind=jnp.bfloat16):
    level = levels(own_key, extent, cuts, -0.22, 0.18) if cuts else 1.0
    entries = jax.random.normal(own_key, extent, jnp.float32) * deviation * level
    return jnp.minimum(jnp.maximum(entries, -reach), reach).astype(kind)


def bell_draw_with(own_key, extent, width, limit, split, heavy, kind=jnp.bfloat16):
    values = width * jax.random.normal(own_key, extent, jnp.float32)
    if split:
        values = values * levels(own_key, extent, split, -0.22, 0.18)
    return jnp.clip(spiked(values, jax.random.fold_in(own_key, 3), *heavy), -limit, limit).astype(kind)


def setup_inputs(seed: int = 0) -> dict:
    key_of = jax.random.split(jax.random.key(seed), 13)
    a_tokens = noise(key_of[0], (TOKENS, D), 1.0, 6.0, ((0, 1024),))
    a_ids = distinct(key_of[1], TOKENS, EXPERTS, TOP, 768)
    a_gates = jnp.clip(jnp.exp(math.log(0.6) - 2.4849067 * jax.random.uniform(key_of[2], (TOKENS, TOP), jnp.float32) ** levels(key_of[2], (TOKENS, TOP), ((0, 1024),), -0.2, 0.2)), 0.05, 0.6)
    a_valid = touch_ends((jax.random.randint(key_of[3], (TOKENS,), 0, 8) < 7).astype(jnp.int32), jax.random.fold_in(key_of[3], 1), 0, 1)
    b_cot = bell_draw_with(key_of[4], (TOKENS, D), (4.0 / (N_REPLICA * TOK_DEV * TOP) ** 0.5), 1.25, ((0, 1024),), (0, 1, 1024, 6.0))
    b_ids = distinct(key_of[5], TOKENS, EXPERTS, TOP, 768)
    b_gates = jnp.clip(jnp.exp(math.log(0.6) - 2.4849067 * jax.random.uniform(key_of[6], (TOKENS, TOP), jnp.float32) ** levels(key_of[6], (TOKENS, TOP), ((0, 1024),), -0.2, 0.2)), 0.05, 0.6)
    b_valid = touch_ends((jax.random.randint(key_of[7], (TOKENS,), 0, 8) < 7).astype(jnp.int32), jax.random.fold_in(key_of[7], 1), 0, 1)
    b_hidden = noise(key_of[8], (EXPERTS, SLOTS, FW), 1.0, 6.0, ((0, 64), (1, 16)))
    w_gate = noise(key_of[9], (EXPERTS, D, FW), D ** -0.5, 0.125, ((0, 64),))
    w_up = noise(key_of[10], (EXPERTS, D, FW), D ** -0.5, 0.125, ((0, 64),))
    w_down = noise(key_of[11], (EXPERTS, FW, D), FW ** -0.5, 0.21875, ((0, 64),))
    return dict(a_tokens=a_tokens, a_ids=a_ids, a_gates=a_gates, a_valid=a_valid, b_cot=b_cot, b_ids=b_ids, b_gates=b_gates, b_valid=b_valid, b_hidden=b_hidden, w_gate=w_gate, w_up=w_up, w_down=w_down)


def slot_keys(expert_ids, valid_mask, experts, capacity):
    top_count = expert_ids.shape[1]
    flat_ids = expert_ids.reshape(-1)
    live = jnp.repeat(valid_mask, top_count) > 0
    onehot = ((flat_ids[:, None] == jnp.arange(experts, dtype=jnp.int32)[None, :]) & live[:, None]).astype(jnp.int32)
    earlier = jnp.cumsum(onehot, axis=0) - onehot
    position = lax.optimization_barrier(jnp.sum(earlier * onehot, axis=1))
    kept_mask = live & (position < capacity)
    return jnp.where(kept_mask, flat_ids * capacity + position, -1).astype(jnp.int32)

def gather_tokens(slot_key, tokens, experts, capacity):
    total = experts * capacity
    tok_count = tokens.shape[0]
    matches = jnp.arange(total, dtype=jnp.int32)[:, None] == slot_key[None, :]
    picker = jnp.any(matches.reshape(total, tok_count, -1), axis=2).astype(jnp.bfloat16)
    sent = jnp.dot(picker, tokens, preferred_element_type=jnp.float32).astype(jnp.bfloat16)
    return sent.reshape(experts, capacity, tokens.shape[1])

def gated_slots(slot_key, gate_values, cotangent, experts, capacity):
    total = experts * capacity
    tok_count = cotangent.shape[0]
    flat_gates = gate_values.reshape(-1)
    matches = jnp.arange(total, dtype=jnp.int32)[:, None] == slot_key[None, :]
    picker = jnp.any(matches.reshape(total, tok_count, -1), axis=2).astype(jnp.bfloat16)
    copied = jnp.dot(picker, cotangent, preferred_element_type=jnp.float32)
    slot_gate = lax.optimization_barrier(jnp.sum(jnp.where(matches, flat_gates[None, :], jnp.zeros_like(flat_gates)[None, :]), axis=1))
    slots = copied * slot_gate[:, None]
    return slots.astype(jnp.bfloat16).reshape(experts, capacity, cotangent.shape[1])

def combine_slots(slot_key, gate_values, returned):
    model_width = returned.shape[-1]
    flat_rows = returned.reshape(-1, model_width)
    picked = flat_rows[jnp.maximum(slot_key, 0)]
    flat_gates = gate_values.reshape(-1)
    scale = jnp.where(slot_key >= 0, flat_gates, jnp.zeros_like(flat_gates))
    summed = picked.astype(flat_gates.dtype) * scale[:, None]
    return lax.optimization_barrier(jnp.sum(summed.reshape(gate_values.shape[0], gate_values.shape[1], model_width), axis=1)).astype(jnp.bfloat16)

def expert_ffn(inputs, gate_weight, up_weight, down_weight):
    model_width = inputs.shape[-1]
    rows = inputs.reshape(-1, model_width)
    gate_proj = jnp.dot(rows, gate_weight, preferred_element_type=jnp.float32)
    up_proj = jnp.dot(rows, up_weight, preferred_element_type=jnp.float32)
    hidden = (jax.nn.silu(gate_proj) * up_proj).astype(jnp.bfloat16)
    result = jnp.dot(hidden, down_weight, preferred_element_type=jnp.float32).astype(jnp.bfloat16)
    return result.reshape(inputs.shape[:-1] + (down_weight.shape[1],))

def group_view(array):
    return jnp.swapaxes(array.reshape((N_EXPERT, N_REPLICA, TOK_DEV) + array.shape[1:]), 0, 1)

def reference(a_tokens, a_ids, a_gates, a_valid, b_cot, b_ids, b_gates, b_valid, b_hidden, w_gate, w_up, w_down):
    hidden_groups = jnp.swapaxes(b_hidden.reshape(EXPERTS, N_REPLICA, N_EXPERT * CAP, FW), 0, 1)
    pieces_all = (group_view(a_tokens), group_view(a_ids), group_view(a_gates), group_view(a_valid), group_view(b_cot), group_view(b_ids), group_view(b_gates), group_view(b_valid), hidden_groups)
    make_keys = partial(slot_keys, experts=EXPERTS, capacity=CAP)
    make_sends = partial(gather_tokens, experts=EXPERTS, capacity=CAP)
    make_slots = partial(gated_slots, experts=EXPERTS, capacity=CAP)

    def run_expert(item):
        return expert_ffn(item[0], item[1], item[2], item[3])

    def expert_grad(item):
        return jnp.dot(item[0].T, item[1], preferred_element_type=jnp.float32)

    def one_group(running, pieces):
        a_tok, a_id, a_gate, a_live, b_tan, b_id, b_gate, b_live, b_hid = pieces
        a_keys = jax.vmap(make_keys)(a_id, a_live)
        sends = jax.vmap(make_sends)(a_keys, a_tok)
        arriving = jnp.swapaxes(sends, 0, 1)
        outputs = lax.map(run_expert, (arriving, w_gate, w_up, w_down))
        returned = jnp.swapaxes(outputs, 0, 1)
        group_out = jax.vmap(combine_slots)(a_keys, a_gate, returned)
        b_keys = jax.vmap(make_keys)(b_id, b_live)
        slots = jax.vmap(make_slots)(b_keys, b_gate, b_tan)
        per_expert = jnp.swapaxes(slots, 0, 1).reshape(EXPERTS, N_EXPERT * CAP, D)
        partial_grad = lax.map(expert_grad, (b_hid, per_expert))
        rounded = lax.optimization_barrier(partial_grad.astype(jnp.bfloat16)).astype(jnp.float32)
        return (running + rounded, group_out)
    start = jnp.zeros((EXPERTS, FW, D), jnp.float32)
    gradient, outs = lax.scan(one_group, start, pieces_all)
    a_out = jnp.swapaxes(outs, 0, 1).reshape(-1, D)
    return (a_out, gradient)
```

```python
import functools
import jax
import jax.numpy as jnp
from jax import lax
from jax.experimental import pallas as pl
from jax.experimental.pallas import tpu as pltpu
from jax.sharding import PartitionSpec as P

MESH = pl.DeviceIdType.MESH
BF16, F32, I32 = jnp.bfloat16, jnp.float32, jnp.int32
NX, NY, NZ, NC = 4, 4, 2, 2
SLOT = 8
OFFSET = 8
CHUNKS = 2


def dot(lhs, rhs, left, right):
    return lax.dot_general(lhs, rhs, (((left,), (right,)), ((), ())), preferred_element_type=F32)


def iota(shape, dim):
    return lax.broadcasted_iota(I32, shape, dim)


def slot_table(ids, gates, valid, planes, capacity):
    top, tokens = ids.shape
    experts = planes * NX
    expert = iota((experts, tokens), 0)
    chosen = jnp.zeros((experts, tokens), F32)
    gate = jnp.zeros((experts, tokens), F32)
    for k in range(top):
        here = ids[k : k + 1, :] == expert
        chosen = jnp.where(here, 1.0, chosen)
        gate = jnp.where(here, gates[k : k + 1, :], gate)
    live = jnp.where(valid > 0, chosen, 0.0)
    earlier = (iota((tokens, tokens), 0) < iota((tokens, tokens), 1)).astype(F32).astype(BF16)
    position = dot(live.astype(BF16), earlier, 1, 0)
    position = jnp.where(live > 0, position, 127.0)
    token = (iota((experts, tokens), 1) + 1).astype(F32)
    lane = iota((experts, 128), 1)
    mine = lax.rem(iota((experts, 128), 0), NX) == lax.rem(lane // 16, 4)
    spread = jnp.zeros((experts, 128), F32)
    for c in range(capacity):
        here = position == float(c)
        who = jnp.sum(jnp.where(here, token, 0.0), axis=1, keepdims=True)
        weight = jnp.sum(jnp.where(here, gate, 0.0), axis=1, keepdims=True)
        at_c = mine & (lax.rem(lane, 16) == c)
        spread = jnp.where(at_c, jnp.where(lane < 64, who, weight), spread)
    plane_of = (iota((planes, experts), 1) // NX == iota((planes, experts), 0)).astype(F32)
    return lax.dot_general(
        plane_of, spread, (((1,), (0,)), ((), ())), precision=lax.Precision.HIGHEST, preferred_element_type=F32
    )


def pair_masks(row0, row1, tokens):
    row1 = pltpu.roll(row1, SLOT, 1)
    token = (iota((tokens, 128), 0) + 1).astype(F32)
    hit0, hit1 = token == row0, token == row1
    pick = jnp.concatenate([jnp.where(hit0, 1.0, 0.0), jnp.where(hit1, 1.0, 0.0)], axis=0)[:, :64]
    gate0, gate1 = pltpu.roll(row0, 64, 1), pltpu.roll(row1, 64, 1)
    gate = jnp.concatenate([jnp.where(hit0, gate0, 0.0), jnp.where(hit1, gate1, 0.0)], axis=0)[:, :64]
    return pick, gate


def split(value):
    high = value.astype(BF16)
    return high, (value - high.astype(F32)).astype(BF16)


def kernel(
    ZL,
    a_tok, a_ids, a_gates, a_valid, b_cot, b_ids, b_gates, b_valid, b_hid, w_gate, w_up, w_down,
    out_a, out_g,
    agA, tabA, agB, tabB, stA, stB, xA, xB, hid, yo, yb, lsend, lrecv, rsend, rrecv,
    wg, wu, wd, hT, hP, part, crecv, csum, yr1, yr2, zs, zr, own,
    local, sA, rA, stabA, rtabA, sB, rB, stabB, rtabB, sxA, rxA, sxB, rxB, sy, ry, sR, rR, sC, rC, sY1, rY1, sY2, rY2, sZ, rZ,
):
    NP = ZL // 2
    T, D = a_tok.shape
    F = w_down.shape[1]
    NB = NZ * NY
    capacity = b_hid.shape[2] // (ZL * NX)
    ring = ZL * NZ
    e, r = lax.axis_index("expert"), lax.axis_index("replica")
    z, x = e // NX, lax.rem(e, NX)
    zh, y, c = r // (NY * NC), lax.rem(r // NC, NY), lax.rem(r, NC)
    place = zh * ZL + z

    def device(place_, x_, y_, c_):
        place_ = lax.rem(place_ + ring, ring)
        return (lax.rem(place_, ZL) * NX + x_, (place_ // ZL * NY + y_) * NC + c_)

    up, down = device(place + 1, x, y, c), device(place - 1, x, y, c)
    side = [None] + [device(place, lax.rem(x + d, NX), y, c) for d in range(1, NX)]
    partner = device(place, x, y, 1 - c)
    y_up, y_down = device(place, x, lax.rem(y + 1, NY), c), device(place, x, lax.rem(y + NY - 1, NY), c)
    far = device(place + ZL, x, y, c)

    def send(src, dst, s, r_, to):
        return pltpu.make_async_remote_copy(
            src_ref=src, dst_ref=dst, send_sem=s, recv_sem=r_, device_id=to, device_id_type=MESH
        )

    rows = T // CHUNKS

    def part_rows(k):
        return pl.ds(k * rows, rows)

    loads = [
        pltpu.make_async_copy(a_tok, agA.at[0, 1], local.at[0]),
        pltpu.make_async_copy(b_cot, agB.at[z], local.at[1]),
        pltpu.make_async_copy(b_hid.at[0], hT, local.at[2]),
        pltpu.make_async_copy(w_gate.at[0], wg, local.at[3]),
        pltpu.make_async_copy(w_up.at[0], wu, local.at[4]),
        pltpu.make_async_copy(w_down.at[0], wd, local.at[5]),
    ]
    for load in loads:
        load.start()

    barrier = pltpu.get_barrier_semaphore()
    peers = [up, down, *side[1:], partner, y_up, y_down, far]
    for peer in peers:
        pl.semaphore_signal(barrier, inc=1, device_id=peer, device_id_type=MESH)
    pl.semaphore_wait(barrier, len(peers))

    def a_up(n, k):
        return send(agA.at[n, 0, part_rows(k)], agA.at[n + 1, 0, part_rows(k)], sA.at[0, n + 1, k], rA.at[0, n + 1, k], up)

    def a_up_first(k):
        return send(agA.at[0, 1, part_rows(k)], agA.at[0, 0, part_rows(k)], sA.at[0, 0, k], rA.at[0, 0, k], up)

    def a_down(n, k):
        return send(agA.at[n, 1, part_rows(k)], agA.at[n + 1, 1, part_rows(k)], sA.at[1, n + 1, k], rA.at[1, n + 1, k], down)

    def ta_up(n):
        return send(tabA.at[n, 0], tabA.at[n + 1, 0], stabA.at[0, n + 1], rtabA.at[0, n + 1], up)

    def ta_up_first():
        return send(tabA.at[0, 1], tabA.at[0, 0], stabA.at[0, 0], rtabA.at[0, 0], up)

    def ta_down(n):
        return send(tabA.at[n, 1], tabA.at[n + 1, 1], stabA.at[1, n + 1], rtabA.at[1, n + 1], down)

    def b_send(way, s, k):
        return send(agB.at[s, part_rows(k)], agB.at[s, part_rows(k)], sB.at[way, s, k], rB.at[s, k], (up, down)[way])

    def tb_send(way, s):
        return send(tabB.at[s], tabB.at[s], stabB.at[way, s], rtabB.at[s], (up, down)[way])

    def x_send(stage, arrived, ss, rr, n, d):
        return send(stage.at[n, lax.rem(x + d, NX)], arrived.at[n, x], ss.at[n, d - 1], rr.at[n, d - 1], side[d])

    def x_wait(stage, arrived, ss, rr, n, d):
        return send(stage.at[n, x], arrived.at[n, lax.rem(x + NX - d, NX)], ss.at[n, d - 1], rr.at[n, d - 1], side[d])

    loads[1].wait()
    for k in range(CHUNKS):
        @pl.when(z < ZL - 1)
        def _():
            b_send(0, z, k).start()

        @pl.when(z > 0)
        def _():
            b_send(1, z, k).start()

    loads[0].wait()
    if OFFSET == 0:
        for k in range(CHUNKS):
            a_up_first(k).start()
            a_down(0, k).start()
    tabB[z] = slot_table(b_ids[...], b_gates[...], b_valid[...], ZL, capacity)

    @pl.when(z < ZL - 1)
    def _():
        tb_send(0, z).start()

    @pl.when(z > 0)
    def _():
        tb_send(1, z).start()

    tabA[0, 1] = slot_table(a_ids[...], a_gates[...], a_valid[...], ZL, capacity)
    if OFFSET == 0:
        ta_up_first().start()
        ta_down(0).start()

    loads[2].wait()
    wide = NP * NX * 2 * SLOT
    col = iota((1, wide), 1)
    slot = lax.rem(col, SLOT)
    source = (2 * (col // (NX * 2 * SLOT)) + lax.rem(col // SLOT, 2)) * NX + lax.rem(col // (2 * SLOT), NX)
    column = jnp.where(slot < capacity, source * capacity + slot, -1)
    mover = (iota((hT.shape[1], wide), 0) == column).astype(F32).astype(BF16)
    hP[...] = dot(hT[...], mover, 1, 0).astype(BF16)
    for load in loads[3:]:
        load.wait()

    tile = min(512, D)

    def columns(n):
        return pl.ds(pl.multiple_of(n * tile, tile), tile)

    def pick_a(n):
        pick, _ = pair_masks(tabA[n, 0, pl.ds(z, 1), :], tabA[n, 1, pl.ds(z, 1), :], T)
        pick = pick.astype(BF16)

        def one(q, _):
            block = agA[n, :, :, columns(q)].reshape(2 * T, tile)
            stA[n, :, :, columns(q)] = dot(pick, block, 0, 0).astype(BF16).reshape(NX, 2 * SLOT, tile)
            return 0

        lax.fori_loop(0, D // tile, one, 0)
        for d in range(1, NX):
            x_send(stA, xA, sxA, rxA, n, d).start()
        xA[n, x] = stA[n, x]

    def pick_b(m):
        _, gate = pair_masks(tabB[2 * m, pl.ds(z, 1), :], tabB[2 * m + 1, pl.ds(z, 1), :], T)
        high, low = split(gate)

        def one(q, _):
            block = agB[pl.ds(2 * m, 2), :, columns(q)].reshape(2 * T, tile)
            rows_ = dot(high, block, 0, 0) + dot(low, block, 0, 0)
            stB[m, :, :, columns(q)] = rows_.astype(BF16).reshape(NX, 2 * SLOT, tile)
            return 0

        lax.fori_loop(0, D // tile, one, 0)
        for d in range(1, NX):
            x_send(stB, xB, sxB, rxB, m, d).start()
        xB[m, x] = stB[m, x]

    f_tiles = [(f, min(256, F - f)) for f in range(0, F, 256)]

    def experts(n, count):
        for q in range(count):
            for d in range(1, NX):
                x_wait(stA, xA, sxA, rxA, n + q, d).wait_recv()
        size = count * NX * 2 * SLOT
        inputs = xA[pl.ds(n, count)].reshape(size, D)
        for f, width in f_tiles:
            gate = dot(inputs, wg[f : f + width, :], 1, 1)
            lift = dot(inputs, wu[f : f + width, :], 1, 1)
            hid[:, f : f + width] = (gate / (1.0 + jnp.exp(-gate)) * lift).astype(BF16)

        def one(q, _):
            result = dot(hid[...], wd[:, columns(q)], 1, 0).astype(BF16)
            yo[pl.ds(n, count), :, :, columns(q)] = result.reshape(count, NX, 2 * SLOT, tile)
            return 0

        lax.fori_loop(0, D // tile, one, 0)
        for q in reversed(range(count)):
            for d in range(1, NX):
                x_send(yo, yb, sy, ry, n + q, d).start()
            yb[n + q, x] = yo[n + q, x]

    half = D // 2
    sub = min(512, half)

    def l_send(n, h):
        return send(lsend.at[n, h], lrecv.at[n, h], sR.at[0, n, h], rR.at[0, n, h], down)

    def r_send(n, h):
        return send(rsend.at[n, h], rrecv.at[n, h], sR.at[1, n, h], rR.at[1, n, h], up)

    def combine(n, first, last):
        for d in range(1, NX):
            x_wait(yo, yb, sy, ry, n, d).wait_recv()
        _, gate = pair_masks(tabA[n, 0, pl.ds(z, 1), :], tabA[n, 1, pl.ds(z, 1), :], T)
        high, low = split(gate)
        for h in range(2):
            sums = []
            for q in range(half // sub):
                block = yb[n, :, :, h * half + q * sub : h * half + (q + 1) * sub].reshape(NX * 2 * SLOT, sub)
                sums.append(dot(high, block, 1, 0) + dot(low, block, 1, 0))
            if not first:
                l_send(n + 1, h).wait_recv()
            for q, value in enumerate(sums):
                at = slice(q * sub, (q + 1) * sub)
                total = value[:T]
                if not first:
                    total = total + lrecv[n + 1, h, :, at].astype(F32)
                lsend[n, h, :, at] = total.astype(BF16)
            l_send(n, h).start()
            if not first:
                r_send(n + 1, h).wait_recv()
            if last:
                l_send(n, h).wait_recv()
            for q, value in enumerate(sums):
                at = slice(q * sub, (q + 1) * sub)
                total = value[T:]
                if not first:
                    total = total + rrecv[n + 1, h, :, at].astype(F32)
                if last:
                    total = total + lrecv[n, h, :, at].astype(F32)
                    out_a[:, h * half + q * sub : h * half + (q + 1) * sub] = total.astype(BF16)
                else:
                    rsend[n, h, :, at] = total.astype(BF16)
            if not last:
                r_send(n, h).start()

    turns = [(h, d) for h in range(2) for d in (2, 1, NY - 1, 0)]

    def block_of(h, d):
        half_of = (1 - zh) if h == 0 else zh
        return half_of * NY + lax.rem(y + d, NY)

    def core_send(b):
        return send(part.at[b, 1 - c], crecv.at[b], sC.at[b], rC.at[b], partner)

    FH = F // 2

    def y1_send(h, way):
        at = pl.ds(way * FH, FH)
        return send(csum.at[block_of(h, 2), at], yr1.at[h, way], sY1.at[h, way], rY1.at[h, way], (y_up, y_down)[way])

    def y2_send(h, way):
        return send(csum.at[block_of(h, (1, NY - 1)[way])], yr2.at[h, way], sY2.at[h, way], rY2.at[h, way], (y_up, y_down)[way])

    def z_send():
        return send(zs, zr, sZ, rZ, far)

    def gradient_blocks():
        for n in range(NP):
            for d in range(1, NX):
                x_wait(stB, xB, sxB, rxB, n, d).wait_recv()
        for h, d in turns:
            b = block_of(h, d)
            cot = xB[:, :, :, pl.ds(pl.multiple_of(b * 256, 256), 256)].reshape(wide, 256)
            value = dot(hP[...], cot, 1, 0)
            part[b, 0] = value[:, :128].astype(BF16)
            part[b, 1] = value[:, 128:].astype(BF16)
            core_send(b).start()

    def core_sums(h):
        for d in (2, 1, NY - 1, 0):
            b = block_of(h, d)
            core_send(b).wait_recv()
            csum[b] = (part[b, c].astype(F32) + crecv[b].astype(F32)).astype(BF16)
            if d == 2:
                for way in range(2):
                    y1_send(h, way).start()

    def y_sums(h):
        for way in range(2):
            b = block_of(h, (1, NY - 1)[way])
            at = pl.ds(way * FH, FH)
            y1_send(h, way).wait_recv()
            csum[b, at] = (csum[b, at].astype(F32) + yr1[h, way].astype(F32)).astype(BF16)
            y2_send(h, way).start()

    def y_last(h):
        for way in range(2):
            y2_send(h, way).wait_recv()
        total = csum[block_of(h, 0)].astype(F32) + yr2[h, 0].astype(F32) + yr2[h, 1].astype(F32)
        if h == 0:
            zs[...] = total.astype(BF16)
            z_send().start()
        else:
            own[...] = total

    B_LAST = ZL - 1
    A_END = OFFSET + 2 * NP + 1

    def step(j, _):
        i = j - OFFSET
        for k in range(CHUNKS):
            @pl.when((j <= B_LAST) & (z - j >= 0))
            def _():
                b_send(0, z - j, k).wait_recv()

                @pl.when(z < ZL - 1)
                def _():
                    b_send(0, z - j, k).start()

            @pl.when((j <= B_LAST) & (z + j < ZL))
            def _():
                b_send(1, z + j, k).wait_recv()

                @pl.when(z > 0)
                def _():
                    b_send(1, z + j, k).start()

            if OFFSET > 0:
                @pl.when(i == 0)
                def _():
                    a_up_first(k).start()
                    a_down(0, k).start()

            @pl.when((i >= 1) & (i <= NP))
            def _():
                send(agA.at[i - 1, 0, part_rows(k)], agA.at[i - 1, 0, part_rows(k)], sA.at[0, i - 1, k], rA.at[0, i - 1, k], up).wait_recv()

                @pl.when(i < NP)
                def _():
                    a_up(i - 1, k).start()
                    a_down(i - 1, k).wait_recv()

                @pl.when(i < NP - 1)
                def _():
                    a_down(i, k).start()

        @pl.when((j <= B_LAST) & (z - j >= 0))
        def _():
            tb_send(0, z - j).wait_recv()

            @pl.when(z < ZL - 1)
            def _():
                tb_send(0, z - j).start()

        @pl.when((j <= B_LAST) & (z + j < ZL))
        def _():
            tb_send(1, z + j).wait_recv()

            @pl.when(z > 0)
            def _():
                tb_send(1, z + j).start()

        if OFFSET > 0:
            @pl.when(i == 0)
            def _():
                ta_up_first().start()
                ta_down(0).start()

        @pl.when((i >= 1) & (i <= NP))
        def _():
            send(tabA.at[i - 1, 0], tabA.at[i - 1, 0], stabA.at[0, i - 1], rtabA.at[0, i - 1], up).wait_recv()

            @pl.when(i < NP)
            def _():
                ta_up(i - 1).start()
                ta_down(i - 1).wait_recv()

            @pl.when(i < NP - 1)
            def _():
                ta_down(i).start()

        even = 1 - lax.rem(z + j, 2)
        whole = even * ((z - j + 2 * ZL) // 2 - ZL) + (1 - even) * ((z + j - 1) // 2)

        @pl.when((j <= B_LAST) & (whole >= 0) & (whole < NP))
        def _():
            pick_b(whole)

        @pl.when((i >= 1) & (i <= NP))
        def _():
            pick_a(i - 1)

        @pl.when((i >= 3) & (i <= NP + 1) & (lax.rem(i + 2, 2) == 1))
        def _():
            experts(i - 3, 2)

        @pl.when(i == NP + 2)
        def _():
            combine(NP - 1, True, False)

        @pl.when((i > NP + 2) & (i < 2 * NP + 1))
        def _():
            combine(2 * NP + 1 - i, False, False)

        @pl.when(j == B_LAST + 1)
        def _():
            gradient_blocks()

        @pl.when(j == B_LAST + 2)
        def _():
            core_sums(0)
            core_sums(1)

        @pl.when(j == B_LAST + 3)
        def _():
            y_sums(0)
            y_sums(1)

        @pl.when(j == B_LAST + 4)
        def _():
            y_last(0)
            y_last(1)

        return 0

    lax.fori_loop(1, max(A_END, B_LAST + 5), step, 0)
    combine(0, NP == 1, True)
    z_send().wait_recv()
    out_g[0] = own[...] + zr[...].astype(F32)

    for k in range(CHUNKS):
        a_up_first(k).wait_send()
    ta_up_first().wait_send()

    def done_a(n, _):
        for k in range(CHUNKS):
            a_up(n, k).wait_send()
        ta_up(n).wait_send()
        return 0

    lax.fori_loop(0, NP - 1, done_a, 0)

    def done_down(n, _):
        for k in range(CHUNKS):
            a_down(n, k).wait_send()
        ta_down(n).wait_send()
        return 0

    lax.fori_loop(0, NP - 1, done_down, 0)

    def done_b(s, _):
        @pl.when((s <= z) & (z < ZL - 1))
        def _():
            for k in range(CHUNKS):
                b_send(0, s, k).wait_send()
            tb_send(0, s).wait_send()

        @pl.when((s >= z) & (z > 0))
        def _():
            for k in range(CHUNKS):
                b_send(1, s, k).wait_send()
            tb_send(1, s).wait_send()

        return 0

    lax.fori_loop(0, ZL, done_b, 0)

    def done_pairs(n, _):
        for d in range(1, NX):
            x_send(stA, xA, sxA, rxA, n, d).wait_send()
            x_send(stB, xB, sxB, rxB, n, d).wait_send()
            x_send(yo, yb, sy, ry, n, d).wait_send()
        for h in range(2):
            l_send(n, h).wait_send()

            @pl.when(n > 0)
            def _():
                r_send(n, h).wait_send()

        return 0

    lax.fori_loop(0, NP, done_pairs, 0)

    def done_blocks(b, _):
        core_send(b).wait_send()
        return 0

    lax.fori_loop(0, NB, done_blocks, 0)
    for h in range(2):
        for way in range(2):
            y1_send(h, way).wait_send()
            y2_send(h, way).wait_send()
    z_send().wait_send()


def body(a_tokens, a_ids, a_gates, a_valid, b_cot, b_ids, b_gates, b_valid, b_hidden, w_gate, w_up, w_down):
    ZL = lax.axis_size("expert") // NX
    NP = ZL // 2
    T, D = a_tokens.shape
    F = w_down.shape[1]
    NB = NZ * NY
    wide = NP * NX * 2 * SLOT
    whole, vmem, dma = pl.BlockSpec(memory_space=pl.ANY), pl.BlockSpec(memory_space=pltpu.VMEM), pltpu.SemaphoreType.DMA
    tab = lambda *lead: pltpu.VMEM((*lead, ZL, 128), F32)
    slots = pltpu.VMEM((NP, NX, 2 * SLOT, D), BF16)
    moving = pltpu.VMEM((NP, 2, T, D // 2), BF16)
    scratch = [
        pltpu.VMEM((NP, 2, T, D), BF16), tab(NP, 2), pltpu.VMEM((ZL, T, D), BF16), tab(ZL),
        slots, slots, slots, slots, pltpu.VMEM((2 * NX * 2 * SLOT, F), BF16), slots, slots,
        moving, moving, moving, moving,
        pltpu.VMEM((F, D), BF16), pltpu.VMEM((F, D), BF16), pltpu.VMEM((F, D), BF16),
        pltpu.VMEM((F, b_hidden.shape[1]), BF16), pltpu.VMEM((F, wide), BF16),
        pltpu.VMEM((NB, NC, F, 128), BF16), pltpu.VMEM((NB, F, 128), BF16), pltpu.VMEM((NB, F, 128), BF16),
        pltpu.VMEM((2, 2, F // 2, 128), BF16), pltpu.VMEM((2, 2, F, 128), BF16),
        pltpu.VMEM((F, 128), BF16), pltpu.VMEM((F, 128), BF16), pltpu.VMEM((F, 128), F32),
        dma((6,)),
        dma((2, NP, CHUNKS)), dma((2, NP, CHUNKS)), dma((2, NP)), dma((2, NP)),
        dma((2, ZL, CHUNKS)), dma((ZL, CHUNKS)), dma((2, ZL)), dma((ZL,)),
        dma((NP, NX - 1)), dma((NP, NX - 1)), dma((NP, NX - 1)), dma((NP, NX - 1)), dma((NP, NX - 1)), dma((NP, NX - 1)),
        dma((2, NP, 2)), dma((2, NP, 2)), dma((NB,)), dma((NB,)),
        dma((2, 2)), dma((2, 2)), dma((2, 2)), dma((2, 2)), dma, dma,
    ]
    return pl.pallas_call(
        functools.partial(kernel, ZL),
        out_shape=(jax.ShapeDtypeStruct((T, D), BF16), jax.ShapeDtypeStruct((1, F, 128), F32)),
        in_specs=[whole, vmem, vmem, vmem, whole, vmem, vmem, vmem, whole, whole, whole, whole],
        out_specs=(vmem, vmem),
        scratch_shapes=scratch,
        compiler_params=pltpu.CompilerParams(
            collective_id=0, has_side_effects=True, vmem_limit_bytes=67_043_328
        ),
    )(
        a_tokens, a_ids.T, a_gates.T, a_valid[None], b_cot, b_ids.T, b_gates.T, b_valid[None],
        jnp.swapaxes(b_hidden, 1, 2), jnp.swapaxes(w_gate, 1, 2), jnp.swapaxes(w_up, 1, 2), w_down,
    )


def solution(mesh):
    tokens, flat = P(("expert", "replica"), None), P(("expert", "replica"))
    weight = P("expert", None, None)
    return jax.shard_map(
        body,
        mesh=mesh,
        in_specs=(
            tokens, tokens, tokens, flat, tokens, tokens, tokens, flat, P("expert", "replica", None), weight, weight, weight,
        ),
        out_specs=(tokens, P("expert", None, "replica")),
        check_vma=False,
    )
```
